16 devices in a mesh: dp: 2 (over y, z), tp: 8 (over x, core).
Axes of the slice: x: 4, y: 2, z: 1, core: 2. Of those that a mesh axis runs over, the one named last changes fastest.
The devices are a block of a 4x4x8 slice.
Arguments:
- x: bfloat16 [2, 4096, 2048], P('dp', 'tp'), parts along dimension 0
- dy: bfloat16 [2, 4096, 2048], P('dp', 'tp'), parts along dimension 0
- wq: bfloat16 [2048, 2048], P(None, 'tp')
- wk: bfloat16 [2048, 2048], P(None, 'tp')
- wv: bfloat16 [2048, 2048], P(None, 'tp')
- wo: bfloat16 [2048, 2048], P('tp')
- w_gate: bfloat16 [2048, 8192], P(None, 'tp')
- w_up: bfloat16 [2048, 8192], P(None, 'tp')
- w_down: bfloat16 [8192, 2048], P('tp')
Outputs:
- output 1: bfloat16 [2, 4096, 2048], P('dp', 'tp'), parts along dimension 0
- output 2: bfloat16 [4096, 2048], P('dp', 'tp'), parts along dimension 0
- output 3: bfloat16 [4096, 2048], P('dp', 'tp'), parts along dimension 0
- output 4: bfloat16 [4096, 2048], P('dp', 'tp'), parts along dimension 0
- output 5: bfloat16 [4096, 2048], P(('dp', 'tp')), parts along dimension 0
- output 6: bfloat16 [4096, 8192], P('dp', 'tp'), parts along dimension 0
- output 7: bfloat16 [4096, 8192], P('dp', 'tp'), parts along dimension 0
- output 8: bfloat16 [16384, 2048], P(('dp', 'tp')), parts along dimension 0
There are 2 independent parts. The reference program is written for one: setup_inputs(seed, part) draws one part's arguments, and reference() takes and returns one part's arrays. A program takes and returns all parts, laid end to end along the dimension named above; an argument that names none is the same for every part.
All inputs are finite; a program needn't handle non-finite values.
Results may differ from the reference program's by a relative error of at most 0.024.
Values are sent between devices in bfloat16 or wider.
A program may use at most 768 MiB of HBM per device.

```python
import jax
import jax.numpy as jnp
from jax import lax

SEQUENCES = 1
TOKENS = 4096
D = 2048
HEADS = 16
KV_HEADS = 16
HEAD = 128
FF = 8192
THETA = 10000
NAMES = ("wq", "wk", "wv", "wo", "w_gate", "w_up", "w_down")
SHAPES = {
    "wq": (D, HEADS * HEAD),
    "wk": (D, KV_HEADS * HEAD),
    "wv": (D, KV_HEADS * HEAD),
    "wo": (HEADS * HEAD, D),
    "w_gate": (D, FF),
    "w_up": (D, FF),
    "w_down": (FF, D),
}


def bump(key, n, height):
    away = (jnp.arange(n, dtype=jnp.int32) - jax.random.randint(key, (), 0, n, jnp.int32)) % n
    return jnp.where(away < n // 8, height, 1.0)


def together(key, own, strength):
    shared = jax.random.normal(key, own.shape[1:], jnp.float32)
    return (own + strength * shared) * lax.rsqrt(1 + strength * strength)


def setup_inputs(seed: int = 0, part: int = 0) -> dict:
    kx, kdy, ka, kb, kz, kf, kh, kl, *kw = jax.random.split(jax.random.key(seed), 8 + len(NAMES))
    kx, kdy, ka, kb = (jax.random.fold_in(k, part) for k in (kx, kdy, ka, kb))
    shape = (SEQUENCES, TOKENS, D)
    much_x, much_dy = jax.random.uniform(kz, (2,), jnp.float32, 0.0, 1.0)
    loud = 2.0 ** jax.random.uniform(jax.random.fold_in(kz, 1), (), jnp.float32, -1.0, 2.0)
    halves = 2.0 ** jax.random.uniform(kl, (2,), jnp.float32, -1.0, 1.0)
    times = {"wq": 1.0, "wk": 1.0, "wv": 2.0, "wo": halves[0], "w_gate": 1.0, "w_up": bump(kh, FF, 4.0), "w_down": halves[1]}
    x = together(ka, jax.random.normal(kx, shape, jnp.float32), much_x) * bump(kf, D, 4.0)
    dy = together(kb, jax.random.normal(kdy, shape, jnp.float32), much_dy)
    drawn = {"x": x.astype(jnp.bfloat16), "dy": (loud * dy * (SEQUENCES * TOKENS) ** -0.5).astype(jnp.bfloat16)}
    for key, name in zip(kw, NAMES, strict=True):
        drawn[name] = (jax.random.normal(key, SHAPES[name], jnp.float32) * SHAPES[name][0] ** -0.5 * times[name]).astype(jnp.bfloat16)
    return drawn


def matmul(a, w):
    return jnp.dot(a, w, preferred_element_type=jnp.float32).astype(jnp.bfloat16)


def normed(h):
    wide = h.astype(jnp.float32)
    scale = lax.rsqrt(jnp.mean(wide**2, -1, keepdims=True) + 1e-6)
    return (wide * scale).astype(jnp.bfloat16)


def turned(t, theta):
    half = t.shape[-1] // 2
    angle = jnp.arange(t.shape[0], dtype=jnp.float32)[:, None] * theta ** (-jnp.arange(half, dtype=jnp.float32) / half)
    cos, sin = jnp.cos(angle)[:, None], jnp.sin(angle)[:, None]
    a, b = t[..., :half].astype(jnp.float32), t[..., half:].astype(jnp.float32)
    return jnp.concatenate([a * cos - b * sin, b * cos + a * sin], -1).astype(jnp.bfloat16)


def seen_by(q, k, v):
    tokens, kv = q.shape[0], k.shape[1]
    q = q.reshape(tokens, kv, -1, q.shape[-1])
    scores = jnp.einsum("tgsd,ugd->gstu", q.astype(jnp.float32), k.astype(jnp.float32)) * q.shape[-1] ** -0.5
    place = jnp.arange(tokens)
    weights = jax.nn.softmax(jnp.where(place[:, None] >= place, scores, -jnp.inf), -1).astype(jnp.bfloat16)
    return jnp.einsum("gstu,ugd->tgsd", weights.astype(jnp.float32), v.astype(jnp.float32)).astype(jnp.bfloat16).reshape(tokens, -1)


def layer(h, w):
    a = normed(h)
    q, k = (turned(matmul(a, w[name]).reshape(h.shape[0], -1, HEAD), THETA) for name in ("wq", "wk"))
    h = h + matmul(seen_by(q, k, matmul(a, w["wv"]).reshape(h.shape[0], -1, HEAD)), w["wo"])
    b = normed(h)
    gate = jnp.dot(b, w["w_gate"], preferred_element_type=jnp.float32)
    up = jnp.dot(b, w["w_up"], preferred_element_type=jnp.float32)
    return h + matmul((jax.nn.silu(gate) * up).astype(jnp.bfloat16), w["w_down"])


def reference(x, dy, wq, wk, wv, wo, w_gate, w_up, w_down):
    weights = dict(zip(NAMES, (wq, wk, wv, wo, w_gate, w_up, w_down), strict=True))

    def take(so_far, sequence):
        h, by_y = sequence
        _, back = jax.vjp(lambda w, h: layer(h, w), weights, h)
        by_weights, by_h = back(by_y)
        return jax.tree.map(lambda total, term: total + term.astype(jnp.float32), so_far, by_weights), by_h

    none_yet = {name: jnp.zeros(w.shape, jnp.float32) for name, w in weights.items()}
    by_weights, by_x = lax.scan(take, none_yet, (x, dy))
    return (by_x, *(by_weights[name].astype(jnp.bfloat16) for name in NAMES))
```

```python
import functools

import jax
import jax.numpy as jnp
from jax import lax
from jax.experimental import pallas as pl
from jax.experimental.pallas import tpu as pltpu
from jax.sharding import PartitionSpec as P

HIDDEN = -2e30
NEG = HIDDEN / 2
LOG2E = 1.4426950408889634
MIB = 2**20
VMEM = 56 * MIB
STRIP = 512
BF, F32 = jnp.bfloat16, jnp.float32


def _dot(a, b, ca=1, cb=0):
    return lax.dot_general(a, b, (((ca,), (cb,)), ((), ())), preferred_element_type=F32)


def _blocks(block, iq, bq):
    strips = range(0, bq, STRIP)
    lax.fori_loop(0, iq * (bq // STRIP), lambda j, _: block(pl.multiple_of(j * STRIP, STRIP), strips, None), None)
    for at in strips:
        block(pl.multiple_of(iq * bq + at, STRIP), [u for u in strips if u >= at], at)


def _visible():
    return lax.broadcasted_iota(jnp.int32, (STRIP, STRIP), 1) >= lax.broadcasted_iota(jnp.int32, (STRIP, STRIP), 0)


def _forward(q_ref, k_ref, v_ref, o_ref, lse_ref, top_s, mix_s):
    heads, bq, d = q_ref.shape
    scale = d**-0.5
    e = scale * LOG2E
    top_s[...] = jnp.full(top_s.shape, NEG, F32)
    mix_s[...] = jnp.zeros(mix_s.shape, F32)
    ones = jnp.ones((mix_s.shape[1] - d, STRIP), BF)

    def block(key, strips, masked):
        here = pl.ds(key, STRIP)
        pieces = [(i, at) for i in range(heads) for at in strips]
        scores = [_dot(k_ref[i, here, :], q_ref[i, at : at + STRIP, :], 1, 1) for i, at in pieces]
        weights, keeps = [], []
        for (i, at), s in zip(pieces, scores):
            if at == masked:
                s = jnp.where(_visible(), s, HIDDEN)
            old = top_s[i : i + 1, at : at + STRIP]
            top = jnp.maximum(old, s.max(axis=0, keepdims=True))
            top_s[i : i + 1, at : at + STRIP] = top
            weights.append(jnp.exp2((s - top) * e).astype(BF))
            keeps.append(jnp.exp2((old - top) * e))
        for (i, at), p, keep in zip(pieces, weights, keeps):
            values = jnp.concatenate([v_ref[i, here, :].T, ones], axis=0)
            mix_s[i, :, at : at + STRIP] = mix_s[i, :, at : at + STRIP] * keep + _dot(values, p)

    _blocks(block, pl.program_id(0), bq)
    for i in range(heads):
        total = mix_s[i, d : d + 1, :]
        o_ref[i] = (mix_s[i, :d, :] * (1 / total)).T.astype(o_ref.dtype)
        lse_ref[i : i + 1, :] = top_s[i : i + 1, :] * scale + jnp.log(total)


def _params(limit=VMEM, **more):
    return pltpu.CompilerParams(dimension_semantics=("arbitrary",), vmem_limit_bytes=limit, **more)


def _whole(shape):
    return pl.BlockSpec(shape, lambda *_: (0,) * len(shape), pipeline_mode=pl.Buffered(1))


def _cost(flops, *arrays):
    return pl.CostEstimate(flops=flops, transcendentals=0, bytes_accessed=sum(a.size * a.dtype.itemsize for a in arrays))


def attend(q, k, v):
    heads, s, d = q.shape
    bq = min(4 * STRIP, s)
    queries = pl.BlockSpec((heads, bq, d), lambda i: (0, i, 0))
    stats = pl.BlockSpec((heads, bq), lambda i: (0, i))
    return pl.pallas_call(
        _forward,
        grid=(s // bq,),
        in_specs=[queries, _whole(k.shape), _whole(v.shape)],
        out_specs=[queries, stats],
        out_shape=[jax.ShapeDtypeStruct(q.shape, q.dtype), jax.ShapeDtypeStruct((heads, s), F32)],
        scratch_shapes=[pltpu.VMEM((heads, bq), F32), pltpu.VMEM((heads, d + 8, bq), F32)],
        compiler_params=_params(),
        cost_estimate=_cost(4 * q.size * s, q, k, v),
        name="attend",
    )(q, k, v)


def _backward(q_ref, k_ref, v_ref, do_ref, lse_ref, delta_ref, dq_ref, dk_ref, dv_ref, dq_s, dk_s, dv_s):
    heads, bq, d = q_ref.shape
    iq = pl.program_id(0)
    scale = d**-0.5
    e = scale * LOG2E

    @pl.when(iq == 0)
    def _():
        dk_s[...] = jnp.zeros_like(dk_s)
        dv_s[...] = jnp.zeros_like(dv_s)

    dq_s[...] = jnp.zeros_like(dq_s)
    lses = [lse_ref[i : i + 1, :] * LOG2E for i in range(heads)]
    deltas = [delta_ref[i : i + 1, :] for i in range(heads)]

    def block(key, strips, masked):
        here = pl.ds(key, STRIP)
        pieces = [(i, at) for i in range(heads) for at in strips]
        qs = [q_ref[i, at : at + STRIP, :] for i, at in pieces]
        dos = [do_ref[i, at : at + STRIP, :] for i, at in pieces]
        scores = [_dot(k_ref[i, here, :], x, 1, 1) for (i, _), x in zip(pieces, qs)]
        dps = [_dot(v_ref[i, here, :], x, 1, 1) for (i, _), x in zip(pieces, dos)]
        for (i, at), s, dp, x, do in zip(pieces, scores, dps, qs, dos):
            p = jnp.exp2(s * e - lses[i][:, at : at + STRIP])
            if at == masked:
                p = jnp.where(_visible(), p, 0.0)
            ds = (p * (dp - deltas[i][:, at : at + STRIP])).astype(BF)
            dv_s[i, here, :] += _dot(p.astype(BF), do)
            dk_s[i, here, :] += _dot(ds, x)
            dq_s[i, :, at : at + STRIP] += _dot(k_ref[i, here, :].T, ds)

    _blocks(block, iq, bq)
    for i in range(heads):
        dq_ref[i] = (dq_s[i] * scale).T.astype(dq_ref.dtype)

    @pl.when(iq == pl.num_programs(0) - 1)
    def _():
        dk_ref[...] = (dk_s[...] * scale).astype(dk_ref.dtype)
        dv_ref[...] = dv_s[...].astype(dv_ref.dtype)


def attend_bwd(q, k, v, d_out, lse, delta):
    heads, s, d = q.shape
    bq = min(2 * STRIP, s)
    queries = pl.BlockSpec((heads, bq, d), lambda i: (0, i, 0))
    stats = pl.BlockSpec((heads, bq), lambda i: (0, i))
    sums = pltpu.VMEM(k.shape, F32)
    return pl.pallas_call(
        _backward,
        grid=(s // bq,),
        in_specs=[queries, _whole(k.shape), _whole(v.shape), queries, stats, stats],
        out_specs=[queries, _whole(k.shape), _whole(v.shape)],
        out_shape=[jax.ShapeDtypeStruct(q.shape, q.dtype)] * 3,
        scratch_shapes=[pltpu.VMEM((heads, d, bq), F32), sums, sums],
        compiler_params=_params(),
        cost_estimate=_cost(10 * q.size * s, q, k, v, d_out),
        name="attend_bwd",
    )(q, k, v, d_out, lse, delta)


HEAD = 128
THETA = 10000
ROWS = 512


def normed(h):
    wide = h.astype(F32)
    scale = lax.rsqrt(jnp.mean(wide**2, -1, keepdims=True) + 1e-6)
    return (wide * scale).astype(BF)


def normed_bwd(h, ct):
    wide, ct = h.astype(F32), ct.astype(F32)
    scale = lax.rsqrt(jnp.mean(wide**2, -1, keepdims=True) + 1e-6)
    return scale * ct - wide * (scale**3 * jnp.mean(ct * wide, -1, keepdims=True))


def tables(tokens):
    lane = jnp.arange(HEAD, dtype=jnp.int32)
    half = HEAD // 2
    rate = THETA ** (-(lane % half).astype(F32) / half)
    run = 64
    far = (jnp.arange(tokens // run, dtype=F32) * run)[:, None, None] * rate
    near = jnp.arange(run, dtype=F32)[:, None] * rate
    far, near = ((jnp.cos(u), jnp.sin(u)) for u in (far, near))
    (cf, sf), (cn, sn) = lax.optimization_barrier((far, near))
    sin = (sf * cn + cf * sn) * jnp.where(lane < half, -1.0, 1.0)
    return (cf * cn - sf * sn).reshape(tokens, HEAD), sin.reshape(tokens, HEAD)


MESH = pl.DeviceIdType.MESH
HALVES = 2


class Ring:
    def __init__(self):
        me = lax.axis_index("tp")
        self.chips = lax.axis_size("tp") // 2
        self.chip, self.core = me // 2, me % 2
        self.me = me

    def dev(self, k, other=0):
        return (self.chip + k) % self.chips * 2 + (self.core + other) % 2

    def greet(self, others=False):
        barrier = pltpu.get_barrier_semaphore()
        to = [self.dev(0, 1), self.dev(1), self.dev(3)] + ([self.dev(1, 1), self.dev(3, 1)] if others else [])
        for one in to:
            pl.semaphore_signal(barrier, inc=1, device_id={"tp": one}, device_id_type=MESH)
        pl.semaphore_wait(barrier, len(to))


def _table(*rows):
    return tuple(tuple(map(int, row)) for row in rows)


def _remote(src, dst, sems, m, to):
    return pltpu.make_async_remote_copy(src_ref=src, dst_ref=dst, send_sem=sems[0].at[m], recv_sem=sems[1].at[m], device_id={"tp": to},
                                        device_id_type=MESH)


class Gather:
    COPIES = _table("0010", "0130", "0001", "0101", "0110", "0030",
                    "3010", "1130", "3001", "1101",
                    "3101", "1001", "2001", "2101")
    EVENTS = ((range(2, 4), ()), (range(2), range(6, 10)), (range(8, 10), ()), (range(4, 6), range(10, 12)), (range(10, 12), ()),
              (range(6, 8), range(12, 14)), (range(12, 14), ()))

    def __init__(self, ring, own, full, send, recv):
        self.ring, self.own, self.full, self.sem = ring, own, full, (send, recv)

    def copy(self, m):
        k, half, to, other = self.COPIES[m]
        place = self.full.at[self.ring.dev(k), half]
        return _remote(self.own.at[half] if k == 0 else place, place, self.sem, m, self.ring.dev(to, other))

    def arrived(self, m):
        k, half, to, other = self.COPIES[m]
        place = self.full.at[self.ring.dev(k - to, other), half]
        _remote(place, place, self.sem, m, self.ring.dev(to, other)).wait_recv()

    def event(self, i):
        for step, (waits, starts) in enumerate(self.EVENTS):
            @pl.when(i == step)
            def _():
                for m in waits:
                    self.arrived(m)
                for m in starts:
                    self.copy(m).start()

    def finish(self):
        for m in range(len(self.COPIES)):
            self.copy(m).wait_send()


def places(ring, i):
    p, other = i // 2, i % 2
    off = (p + 1) // 2
    half = p // 2 - p // 3
    return (ring.dev(ring.chips - off, other), half), (ring.dev(off, other), 1 - half)


def _qkv_kernel(own_ref, wq_ref, wk_ref, wv_ref, cos_ref, sin_ref, wg_ref, wu_ref, wd_ref, full_ref, q_ref, k_ref, v_ref, wt_ref, wgt_ref, wut_ref, wdt_ref,
                a_s, cos_s, sin_s, q_s, k_s, v_s, send, recv, in_sem, out_sem, own_sem):
    ring = Ring()
    gather = Gather(ring, own_ref, full_ref, send, recv)
    i = pl.program_id(0)
    slot = i % 2
    heads, r = q_s.shape[1], own_ref.shape[1]
    mine = [pltpu.make_async_copy(a_s.at[0, s], full_ref.at[ring.me, s], own_sem.at[s]) for s in range(HALVES)]

    def loads(i, slot, from_own):
        out = []
        for s, (dev, half) in enumerate(places(ring, i)):
            src = own_ref.at[s] if from_own else full_ref.at[dev, half]
            out += [pltpu.make_async_copy(src, a_s.at[slot, s], in_sem.at[slot, s]),
                    pltpu.make_async_copy(cos_ref.at[dev, half], cos_s.at[slot, s], in_sem.at[slot, 2 + s]),
                    pltpu.make_async_copy(sin_ref.at[dev, half], sin_s.at[slot, s], in_sem.at[slot, 4 + s])]
        return out

    def stores(i, slot):
        return [pltpu.make_async_copy(buf.at[slot, :, s], ref.at[:, dev, half], out_sem.at[slot, 2 * m + s])
                for s, (dev, half) in enumerate(places(ring, i)) for m, (buf, ref) in enumerate(((q_s, q_ref), (k_s, k_ref), (v_s, v_ref)))]

    @pl.when(i == 0)
    def _():
        ring.greet()
        for m in range(6):
            gather.copy(m).start()
        for u in loads(i, 0, True):
            u.start()
        for m, w_ref in enumerate((wq_ref, wk_ref, wv_ref)):
            wt_ref[m] = w_ref[...].T

    for w_ref, t_ref in ((wg_ref, wgt_ref), (wu_ref, wut_ref), (wd_ref, wdt_ref)):
        t_ref[...] = w_ref[...].T
    for u in loads(i, slot, False):
        u.wait()

    @pl.when(i == 0)
    def _():
        for u in mine:
            u.start()

    @pl.when(i > 1)
    def _():
        for u in stores(i - 2, slot):
            u.wait()

    a = a_s[slot].reshape(HALVES * r, -1)
    cos, sin = cos_s[slot].reshape(-1, HEAD), sin_s[slot].reshape(-1, HEAD)
    for w_ref, out_s in ((wq_ref, q_s), (wk_ref, k_s), (wv_ref, v_s)):
        t = _dot(a, w_ref[...], 1, 0).astype(BF)
        for n in range(heads):
            one = t[:, n * HEAD : (n + 1) * HEAD]
            if out_s is not v_s:
                wide = one.astype(F32)
                one = (wide * cos + pltpu.roll(wide, HEAD // 2, 1) * sin).astype(BF)
            out_s[slot, n] = one.reshape(HALVES, r, HEAD)
    for u in stores(i, slot):
        u.start()

    @pl.when(i == 0)
    def _():
        for u in mine:
            u.wait()

    gather.event(i)

    @pl.when(i < STEPS - 1)
    def _():
        for u in loads(i + 1, 1 - slot, False):
            u.start()

    @pl.when(i == STEPS - 1)
    def _():
        for u in stores(i - 1, 1 - slot) + stores(i, slot):
            u.wait()
        gather.finish()


STEPS = 8
ANY = pl.BlockSpec(memory_space=pl.ANY)


def qkv(own, ws, cos, sin, turn):
    devices, _, r, _ = cos.shape
    d = own.shape[1]
    heads = ws[0].shape[1] // HEAD
    shape = jax.ShapeDtypeStruct((heads, devices, HALVES, r, HEAD), BF)
    full = jax.ShapeDtypeStruct((devices, HALVES, r, d), BF)
    wt = (len(ws), *ws[0].shape[::-1])
    dma = pltpu.SemaphoreType.DMA
    copies = len(Gather.COPIES)
    return pl.pallas_call(
        _qkv_kernel,
        grid=(STEPS,),
        in_specs=[ANY, *(_whole(w.shape) for w in ws), ANY, ANY, *(pl.BlockSpec((w.shape[0], w.shape[1] // STEPS), lambda i: (0, i)) for w in turn)],
        out_specs=[ANY] * 4 + [_whole(wt), *(pl.BlockSpec((w.shape[1] // STEPS, w.shape[0]), lambda i: (i, 0)) for w in turn)],
        out_shape=[full, shape, shape, shape, *(jax.ShapeDtypeStruct(u, BF) for u in (wt, *(w.shape[::-1] for w in turn)))],
        scratch_shapes=[pltpu.VMEM((2, HALVES, r, d), BF), *[pltpu.VMEM((2, HALVES, r, HEAD), F32)] * 2,
                        *[pltpu.VMEM((2, heads, HALVES, r, HEAD), BF)] * 3, dma((copies,)), dma((copies,)), dma((2, 6)), dma((2, 6)), dma((2,))],
        compiler_params=_params(collective_id=0, has_side_effects=True),
        cost_estimate=_cost(6 * devices * own.size * ws[0].shape[1], own, *ws),
        name="gather_qkv",
    )(own.reshape(HALVES, r, d), *ws, cos, sin, *turn)


def _ffn_kernel(own_ref, dy_ref, wg_in, wu_in, wdt_in, wgt_in, wut_in, full_ref, hid_ref, dg_ref, du_ref, db_ref,
                b_s, dy_s, hid_s, dg_s, du_s, db_s, wg_ref, wu_ref, wdt_ref, wgt_ref, wut_ref, send, recv, in_sem, out_sem, own_sem, w_sem):
    ring = Ring()
    gather = Gather(ring, own_ref, full_ref, send, recv)
    i = pl.program_id(0)
    slot = i % 2
    r = own_ref.shape[1]
    mine = [pltpu.make_async_copy(b_s.at[0, s], full_ref.at[ring.me, s], own_sem.at[s]) for s in range(HALVES)]

    weights = [pltpu.make_async_copy(src, dst, w_sem.at[m]) for m, (src, dst) in enumerate(
        ((wg_in, wg_ref), (wu_in, wu_ref), (wdt_in, wdt_ref), (wgt_in, wgt_ref), (wut_in, wut_ref)))]

    def have(*which):
        @pl.when(i == 0)
        def _():
            for m in which:
                weights[m].wait()

    def loads(i, slot, from_own):
        out = []
        for s, (dev, half) in enumerate(places(ring, i)):
            src = own_ref.at[s] if from_own else full_ref.at[dev, half]
            out += [pltpu.make_async_copy(src, b_s.at[slot, s], in_sem.at[slot, s]),
                    pltpu.make_async_copy(dy_ref.at[dev, half], dy_s.at[slot, s], in_sem.at[slot, 2 + s])]
        return out

    def stores(i, slot):
        return [pltpu.make_async_copy(buf.at[slot, s], ref.at[dev, half], out_sem.at[slot, 2 * m + s])
                for s, (dev, half) in enumerate(places(ring, i))
                for m, (buf, ref) in enumerate(((hid_s, hid_ref), (dg_s, dg_ref), (du_s, du_ref), (db_s, db_ref)))]

    @pl.when(i == 0)
    def _():
        ring.greet()
        for m in range(6):
            gather.copy(m).start()
        for u in loads(i, 0, True) + weights:
            u.start()

    for u in loads(i, slot, False):
        u.wait()

    @pl.when(i == 0)
    def _():
        for u in mine:
            u.start()

    b = b_s[slot].reshape(HALVES * r, -1)
    have(0)
    gate = _dot(b, wg_ref[...])
    have(1)
    up = _dot(b, wu_ref[...])
    have(2)
    dh = _dot(dy_s[slot].reshape(HALVES * r, -1), wdt_ref[...], 1, 0).astype(BF).astype(F32)

    @pl.when(i == 0)
    def _():
        for u in mine:
            u.wait()

    gather.event(i)

    @pl.when(i < STEPS - 1)
    def _():
        for u in loads(i + 1, 1 - slot, False):
            u.start()

    @pl.when(i > 1)
    def _():
        for u in stores(i - 2, slot):
            u.wait()

    s = 1 / (1 + jnp.exp(-gate))
    silu = gate * s
    hid_s[slot] = (silu * up).astype(BF).reshape(HALVES, r, -1)
    dg = (dh * up * (s * (1 + gate * (1 - s)))).astype(BF)
    du = (dh * silu).astype(BF)
    dg_s[slot] = dg.reshape(HALVES, r, -1)
    du_s[slot] = du.reshape(HALVES, r, -1)
    have(3, 4)
    db_s[slot] = (_dot(dg, wgt_ref[...], 1, 0) + _dot(du, wut_ref[...], 1, 0)).astype(BF).reshape(HALVES, r, -1)
    for u in stores(i, slot):
        u.start()

    @pl.when(i == STEPS - 1)
    def _():
        for u in stores(i - 1, 1 - slot) + stores(i, slot):
            u.wait()
        gather.finish()


def ffn(own, dy, wg, wu, wgt, wut, wdt):
    devices, _, r, d = dy.shape
    f = wg.shape[1]
    array = lambda k: jax.ShapeDtypeStruct((devices, HALVES, r, k), BF)
    dma = pltpu.SemaphoreType.DMA
    copies = len(Gather.COPIES)
    return pl.pallas_call(
        _ffn_kernel,
        grid=(STEPS,),
        in_specs=[ANY] * 7,
        out_specs=[ANY] * 5,
        out_shape=[array(d), array(f), array(f), array(f), array(d)],
        scratch_shapes=[*[pltpu.VMEM((2, HALVES, r, d), BF)] * 2, *[pltpu.VMEM((2, HALVES, r, f), BF)] * 3, pltpu.VMEM((2, HALVES, r, d), BF),
                        *(pltpu.VMEM(w.shape, BF) for w in (wg, wu, wdt, wgt, wut)),
                        dma((copies,)), dma((copies,)), dma((2, 4)), dma((2, 8)), dma((2,)), dma((5,))],
        compiler_params=_params(collective_id=1, has_side_effects=True),
        cost_estimate=_cost(10 * dy.size * f, own, dy, dy, wg, wu, wdt),
        name="gather_ffn",
    )(own.reshape(HALVES, r, d), dy, wg, wu, wdt, wgt, wut)


class Scatter:
    SENDS = (*_table("201"), *_table("213"), *_table("1110", "3031", "1010", "3131"))
    ORDER = _table("20", "21", "11", "30", "10", "31", "00", "01")
    COPIES = 8 + len(SENDS)

    def __init__(self, ring, part, pair, relay, last, own, send, recv, load):
        self.ring, self.part, self.pair, self.own, self.sem, self.load = ring, part, pair, own, (send, recv), load
        self.buffers = {"relay": relay, "last": last}

    def copy(self, m):
        if m < len(self.ORDER):
            k, half = self.ORDER[m]
            return _remote(self.part.at[self.ring.dev(k, 1), half], self.pair.at[k, half], self.sem, m, self.ring.dev(0, 1))
        k, half, to, *side = self.SENDS[m - len(self.ORDER)]
        dst = self.buffers["last"].at[side[0], half] if side else self.buffers["relay"].at[half]
        return _remote(self.pair.at[k, half], dst, self.sem, m, self.ring.dev(to))

    def own_load(self, m):
        k, half = self.ORDER[m]
        return pltpu.make_async_copy(self.part.at[self.ring.dev(k), half], self.own.at[m % 2], self.load.at[m % 2])

    def begin(self):
        self.ring.greet()
        for m in range(8):
            self.copy(m).start()
        for m in range(2):
            self.own_load(m).start()

    def add(self, m, relayed=None):
        k, half = self.ORDER[m]
        self.copy(m).wait_recv()
        self.own_load(m).wait()
        if relayed is not None:
            self.copy(8 + relayed).wait_recv()
        rows = 32

        def some(j, _):
            here = pl.ds(pl.multiple_of(j * rows, rows), rows)
            total = self.pair[k, half, here].astype(F32) + self.own[m % 2, here].astype(F32)
            if relayed is not None:
                total += self.buffers["relay"][relayed, here].astype(F32)
            self.pair[k, half, here] = total.astype(BF)

        lax.fori_loop(0, self.pair.shape[2] // rows, some, None)
        if m + 2 < 8:
            self.own_load(m + 2).start()

    def first(self):
        for m in range(4):
            self.add(m)
            self.copy(8 + m).start()

    def second(self):
        for m in (4, 5):
            self.add(m, m - 4)
            self.copy(8 + m).start()

    def final(self, out):
        last = self.buffers["last"]
        for half in range(HALVES):
            m = 6 + half
            self.copy(m).wait_recv()
            self.own_load(m).wait()
            self.copy(12 - 2 * half).wait_recv()
            self.copy(11 + 2 * half).wait_recv()
            rows = 32

            def some(j, _):
                here = pl.ds(pl.multiple_of(j * rows, rows), rows)
                total = self.pair[0, half, here].astype(F32) + self.own[m % 2, here].astype(F32)
                out[half, here] = (total + last[0, half, here].astype(F32) + last[1, half, here].astype(F32)).astype(BF)

            lax.fori_loop(0, self.pair.shape[2] // rows, some, None)
        for m in range(self.COPIES):
            self.copy(m).wait_send()


def _scatter_kernel(part_ref, *refs, groups, relay_step):
    outs = sum(len(flips) for _, flips in groups)
    ins = len(groups) + outs
    given, results, out_ref, scratch = refs[:ins], refs[ins : ins + outs], refs[ins + outs], refs[ins + outs + 1 :]
    *scratch, whole_sem = scratch
    scratch, wholes = scratch[:-outs], list(scratch[-outs:])
    ring = Ring()
    scatter = Scatter(ring, part_ref, *scratch)
    i = pl.program_id(0)
    copies, at = [], 0
    for _, flips in groups:
        for m in range(len(flips)):
            copies.append(pltpu.make_async_copy(given[at + 1 + m], wholes[len(copies)], whole_sem.at[len(copies)]))
        at += 1 + len(flips)

    @pl.when(i == 0)
    def _():
        scatter.begin()
        for u in copies:
            u.start()
        scatter.first()
        for u in copies:
            u.wait()

    @pl.when(i == relay_step)
    def _():
        scatter.second()

    first = at = to = 0
    for steps, flips in groups:
        s_ref, r_refs = given[at], wholes[to : to + len(flips)]
        at, results_here, to = at + 1 + len(flips), results[to : to + len(flips)], to + len(flips)

        @pl.when((i >= first) & (i < first + steps))
        def _():
            for r_ref, o_ref, flip in zip(r_refs, results_here, flips):
                o_ref[...] = (_dot(r_ref[...].T, s_ref[...], 1, 0) if flip else _dot(s_ref[...].T, r_ref[...], 1, 0)).astype(BF)

        first += steps

    @pl.when(i == pl.num_programs(0) - 1)
    def _():
        scatter.final(out_ref)


def scattered_beside(part, products, tile, relay_step, collective_id, name):
    devices, _, r, d = part.shape
    groups, given, specs, wholes, out_specs, out_shape, first, flops = [], [], [], [], [], [], 0, 0
    for s, others in products:
        t, n = s.shape
        steps = n // tile
        at = lambda i, first=first, steps=steps: jnp.clip(i - first, 0, steps - 1)
        given.append(s)
        specs.append(pl.BlockSpec((t, tile), lambda i, at=at: (0, at(i))))
        for u, flip in others:
            k = u.shape[1]
            given.append(u)
            specs.append(ANY)
            wholes.append(pltpu.VMEM(u.shape, BF))
            out_shape.append(jax.ShapeDtypeStruct((k, n) if flip else (n, k), BF))
            out_specs.append(pl.BlockSpec((k, tile), lambda i, at=at: (0, at(i))) if flip else pl.BlockSpec((tile, k), lambda i, at=at: (at(i), 0)))
            flops += 2 * t * n * k
        groups.append((steps, tuple(flip for _, flip in others)))
        first += steps
    dma = pltpu.SemaphoreType.DMA
    *results, rows = pl.pallas_call(
        functools.partial(_scatter_kernel, groups=tuple(groups), relay_step=relay_step),
        grid=(first,),
        in_specs=[ANY, *specs],
        out_specs=[*out_specs, pl.BlockSpec((HALVES, r, d), lambda i: (0, 0, 0))],
        out_shape=[*out_shape, jax.ShapeDtypeStruct((HALVES, r, d), BF)],
        scratch_shapes=[pltpu.VMEM((4, HALVES, r, d), BF), pltpu.VMEM((2, r, d), BF), pltpu.VMEM((2, HALVES, r, d), BF), pltpu.VMEM((2, r, d), BF),
                        dma((Scatter.COPIES,)), dma((Scatter.COPIES,)), dma((2,)), *wholes, dma((len(wholes),))],
        compiler_params=_params(63 * MIB, collective_id=collective_id, has_side_effects=True),
        cost_estimate=_cost(flops, part, *given),
        name=name,
    )(part, *given)
    return rows, results


class Exchange:
    NEAR = _table("01", "10", "11", "30", "31")
    FAR = _table("010", "011", "130", "131")
    COPIES = len(NEAR) + 2 * len(FAR)

    def __init__(self, ring, piece, land, relay, send, recv):
        self.ring, self.piece, self.land, self.relay, self.sem = ring, piece, land, relay, (send, recv)
        self.part = relay.shape[2]

    def near(self, m):
        to = self.ring.dev(*self.NEAR[m])
        return _remote(self.piece(to), self.land(self.ring.me), self.sem, m, to)

    def some(self, ref, side):
        return ref.at[pl.ds(side * self.part, self.part)]

    def far(self, m):
        side, k, other = self.FAR[m]
        return _remote(self.some(self.piece(self.ring.dev(2, other)), side), self.relay.at[side, other], self.sem, len(self.NEAR) + m, self.ring.dev(k))

    def on(self, m):
        side, k, other = self.FAR[m]
        return _remote(self.relay.at[side, other], self.some(self.land(self.ring.dev(-k)), side), self.sem,
                       len(self.NEAR) + len(self.FAR) + m, self.ring.dev(k, other))

    def begin(self, k):
        for m in range(len(self.FAR)) if k == 2 else ():
            self.far(m).start()
        for m, (chips, _) in enumerate(self.NEAR):
            if chips == k:
                self.near(m).start()

    def send_on(self):
        for m in range(len(self.FAR)):
            self.far(m).wait_recv()
            self.on(m).start()

    def arrived(self, k):
        for m, (chips, other) in enumerate(self.NEAR):
            if (chips + k) % 4 == 0:
                place = self.land(self.ring.dev(k, other))
                _remote(place, place, self.sem, m, self.ring.dev(chips, other)).wait_recv()
        for m, (side, chips, other) in enumerate(self.FAR if k == 2 else ()):
            place = self.some(self.land(self.ring.dev(2, other)), side)
            _remote(place, place, self.sem, len(self.NEAR) + len(self.FAR) + m, self.ring.dev(chips, other)).wait_recv()

    def finish(self):
        for m in range(len(self.NEAR)):
            self.near(m).wait_send()
        for m in range(len(self.FAR)):
            self.far(m).wait_send()
            self.on(m).wait_send()


ONE = 64
CHIPS = (2, 1, 3, 0)


def _by_rows(total, act):
    lax.fori_loop(0, total // ONE, lambda j, _: act(pl.ds(pl.multiple_of(j * ONE, ONE), ONE)), None)


def _wo_kernel(o_ref, wo_ref, x_ref, mine_ref, h_ref, b_ref, land_s, relay_s, wo_s, sum_s, send, recv, here):
    ring = Ring()
    heads, t = land_s.shape[1], land_s.shape[2]
    exchange = Exchange(ring, lambda dev: o_ref.at[:, dev], lambda dev: land_s.at[dev], relay_s, send, recv)
    own = pltpu.make_async_copy(o_ref.at[:, ring.me], land_s.at[ring.me], here.at[0])
    whole = pltpu.make_async_copy(wo_ref, wo_s, here.at[1])
    whole.start()
    own.start()
    ring.greet(True)
    for k in CHIPS:
        exchange.begin(k)
    whole.wait()
    own.wait()
    wide = 2 * heads * HEAD
    for k in CHIPS[::-1]:
        exchange.arrived(k)
        chip = (ring.chip + k) % ring.chips
        cols = pl.ds(pl.multiple_of(chip * wide, wide), wide)
        mine_ref[:, cols] = jnp.concatenate([land_s[chip * 2 + core, n] for core in range(2) for n in range(heads)], axis=1)
        if k == 0:
            exchange.send_on()
        term = _dot(mine_ref[:, cols], wo_s[cols, :])
        sum_s[...] = term if k == 0 else sum_s[...] + term

    def last(rows):
        h = (x_ref[rows].astype(F32) + sum_s[rows].astype(BF).astype(F32)).astype(BF)
        h_ref[rows] = h
        b_ref[rows] = normed(h)

    _by_rows(t, last)
    exchange.finish()


def exchange_wo(o, wo, x):
    heads, devices, t, _ = o.shape
    d = x.shape[1]
    dma = pltpu.SemaphoreType.DMA
    return pl.pallas_call(
        _wo_kernel,
        in_specs=[ANY, ANY, pl.BlockSpec(memory_space=pltpu.VMEM)],
        out_specs=[pl.BlockSpec(memory_space=pltpu.VMEM)] * 3,
        out_shape=[jax.ShapeDtypeStruct((t, wo.shape[0]), BF), *[jax.ShapeDtypeStruct(x.shape, BF)] * 2],
        scratch_shapes=[pltpu.VMEM((devices, heads, t, HEAD), BF), pltpu.VMEM((2, 2, heads // 2, t, HEAD), BF), pltpu.VMEM(wo.shape, BF),
                        pltpu.VMEM((t, d), F32), dma((Exchange.COPIES,)), dma((Exchange.COPIES,)), dma((2,))],
        compiler_params=pltpu.CompilerParams(vmem_limit_bytes=VMEM, collective_id=4, has_side_effects=True),
        cost_estimate=_cost(2 * t * wo.size, o, x, wo),
        name="exchange_wo",
    )(o, wo, x)


def _dwo_kernel(wo_ref, db_ref, h_ref, dy_ref, mine_ref, dh_ref, do_ref, dwo_ref, out_s, relay_s, wo_s, dwo_s, send, recv, here):
    ring = Ring()
    heads, t = out_s.shape[1], out_s.shape[2]
    exchange = Exchange(ring, lambda dev: out_s.at[dev], lambda dev: do_ref.at[:, dev], relay_s, send, recv)
    own = pltpu.make_async_copy(out_s.at[ring.me], do_ref.at[:, ring.me], here.at[0])
    whole = pltpu.make_async_copy(wo_ref, wo_s, here.at[1])
    whole.start()
    ring.greet(True)

    def first(rows):
        dh_ref[rows] = (dy_ref[rows].astype(F32) + normed_bwd(h_ref[rows], db_ref[rows]).astype(BF).astype(F32)).astype(BF)

    _by_rows(t, first)
    whole.wait()
    wide = 2 * heads * HEAD
    for k in CHIPS:
        chip = (ring.chip + k) % ring.chips
        part = _dot(dh_ref[...], wo_s[pl.ds(pl.multiple_of(chip * wide, wide), wide), :], 1, 1).astype(BF)
        for m in range(2 * heads):
            out_s[chip * 2 + m // heads, m % heads] = part[:, m * HEAD : (m + 1) * HEAD]
        exchange.begin(k)
    own.start()
    tiles = [pl.ds(m, wide) for m in range(0, dwo_s.shape[0], wide)]
    stores = [pltpu.make_async_copy(dwo_s.at[tile], dwo_ref.at[tile], here.at[2 + m]) for m, tile in enumerate(tiles)]
    for m, (tile, store) in enumerate(zip(tiles, stores)):
        dwo_s[tile] = _dot(mine_ref[:, tile].T, dh_ref[...]).astype(BF)
        store.start()
        if m == 0:
            exchange.send_on()
    for k in CHIPS:
        exchange.arrived(k)
    for u in (own, *stores):
        u.wait()
    exchange.finish()


def exchange_dwo(wo, db, h, dy, mine, heads):
    t, d = h.shape
    devices = wo.shape[0] // heads // HEAD
    dma = pltpu.SemaphoreType.DMA
    vmem = pl.BlockSpec(memory_space=pltpu.VMEM)
    return pl.pallas_call(
        _dwo_kernel,
        in_specs=[ANY, *[vmem] * 4],
        out_specs=[vmem, ANY, ANY],
        out_shape=[jax.ShapeDtypeStruct(h.shape, BF), jax.ShapeDtypeStruct((heads, devices, t, HEAD), BF), jax.ShapeDtypeStruct(wo.shape, BF)],
        scratch_shapes=[pltpu.VMEM((devices, heads, t, HEAD), BF), pltpu.VMEM((2, 2, heads // 2, t, HEAD), BF), pltpu.VMEM(wo.shape, BF),
                        pltpu.VMEM(wo.shape, BF), dma((Exchange.COPIES,)), dma((Exchange.COPIES,)), dma((2 + devices // 2,))],
        compiler_params=pltpu.CompilerParams(vmem_limit_bytes=VMEM, collective_id=5, has_side_effects=True),
        cost_estimate=_cost(4 * t * wo.size, wo, wo),
        name="exchange_dwo",
    )(wo, db, h, dy, mine)


def _da_kernel(dq_ref, dk_ref, dv_ref, cos_ref, sin_ref, wt_ref, g_ref, da_ref):
    rows = g_ref.shape[0]
    cos, sin = cos_ref[...].reshape(rows, HEAD), sin_ref[...].reshape(rows, HEAD)
    heads = dq_ref.shape[0]
    for m, ref in enumerate((dq_ref, dk_ref, dv_ref)):
        for n in range(heads):
            one = ref[n].reshape(rows, HEAD)
            if ref is not dv_ref:
                wide = one.astype(F32)
                one = (wide * cos - pltpu.roll(wide, HEAD // 2, 1) * sin).astype(BF)
            g_ref[:, (m * heads + n) * HEAD : (m * heads + n + 1) * HEAD] = one
    da_ref[...] = _dot(g_ref[...], wt_ref[...], 1, 0).astype(BF)


def da_of(dq, dk, dv, cos, sin, wt):
    heads, t, _ = dq.shape
    k, d = wt.shape
    place = pl.BlockSpec((ROWS, HEAD), lambda i: (i, 0))
    return pl.pallas_call(
        _da_kernel,
        grid=(t // ROWS,),
        in_specs=[pl.BlockSpec((heads, ROWS, HEAD), lambda i: (0, i, 0))] * 3 + [place, place, _whole(wt.shape)],
        out_specs=[pl.BlockSpec((ROWS, k), lambda i: (i, 0)), pl.BlockSpec((ROWS, d), lambda i: (i, 0))],
        out_shape=[jax.ShapeDtypeStruct((t, k), BF), jax.ShapeDtypeStruct((t, d), BF)],
        compiler_params=_params(),
        cost_estimate=_cost(2 * t * k * d, wt),
        name="da",
    )(dq, dk, dv, cos, sin, wt)


def gathered(t):
    return lax.all_gather(t, "tp", axis=0, tiled=True)


def scattered(t):
    return lax.psum_scatter(t, "tp", scatter_dimension=0, tiled=True)


def after(t, *first):
    return lax.optimization_barrier((t, *first))[0]


def layer(x, dy, wq, wk, wv, wo, wg, wu, wd):
    t, d = x.shape
    n = lax.axis_size("tp")
    r = t // HALVES
    tokens = n * t
    table = tables(tokens)
    flat = lambda u: u.reshape(tokens, -1)

    a, *q, wt, wgt, wut, wdt = qkv(normed(x), (wq, wk, wv), *(u.reshape(n, HALVES, r, HEAD) for u in table), (wg, wu, wd))
    q, k, v = (u.reshape(-1, tokens, HEAD) for u in q)
    heads = len(q)
    whole_wo = gathered(wo)
    dys = gathered(after(dy, a))
    out, lse = attend(q, k, v)
    mine, h, b = exchange_wo(out.reshape(heads, n, t, HEAD), whole_wo, x)

    b, hid, dg, du, db = ffn(b, dys.reshape(n, HALVES, r, d), wg, wu, wgt, wut, wdt)
    db, (dwg, dwu) = scattered_beside(db, ((flat(b), ((flat(dg), False), (flat(du), False))),), 512, 3, 2, "scatter_db")
    dh, dout, dwo = exchange_dwo(whole_wo, db.reshape(t, d), h, dy, mine, heads)
    dwo = scattered(dwo)
    dout = dout.reshape(heads, tokens, HEAD)
    delta = (dout.astype(F32) * out.astype(F32)).sum(-1)
    g, da = da_of(*attend_bwd(q, k, v, dout, lse, delta), *table, wt.reshape(-1, d))
    da, (dwd, dwqkv) = scattered_beside(da.reshape(n, HALVES, r, d), ((dys, ((flat(hid), True),)), (flat(a), ((g, False),))), 512, 5, 3, "scatter_da")
    dx = dh + normed_bwd(x, da.reshape(t, d)).astype(BF)
    dwq, dwk, dwv = jnp.split(dwqkv, 3, axis=1)
    return dx, dwq, dwk, dwv, dwo, dwg, dwu, dwd


def solution(mesh):
    def step(x, dy, *weights):
        dx, *dw = layer(x[0], dy[0], *weights)
        return (dx[None], *dw)

    states, by_columns, by_rows = P("dp", "tp", None), P(None, "tp"), P("tp", None)
    weights = (by_columns, by_columns, by_columns, by_rows, by_columns, by_columns, by_rows)
    own = tuple(P("dp", "tp") if spec == by_columns else P(("dp", "tp"), None) for spec in weights)
    return jax.shard_map(step, mesh=mesh, in_specs=(states, states, *weights), out_specs=(states, *own), check_vma=False)
```

```python
import functools

import jax
import jax.numpy as jnp
from jax import lax
from jax.experimental import pallas as pl
from jax.experimental.pallas import tpu as pltpu
from jax.sharding import PartitionSpec as P

HIDDEN = -2e30
NEG = HIDDEN / 2
LOG2E = 1.4426950408889634
MIB = 2**20
VMEM = 56 * MIB
STRIP = 512
BF, F32 = jnp.bfloat16, jnp.float32


def _dot(a, b, ca=1, cb=0):
    return lax.dot_general(a, b, (((ca,), (cb,)), ((), ())), preferred_element_type=F32)


def _blocks(block, iq, bq):
    strips = range(0, bq, STRIP)
    lax.fori_loop(0, iq * (bq // STRIP), lambda j, _: block(pl.multiple_of(j * STRIP, STRIP), strips, None), None)
    for at in strips:
        block(pl.multiple_of(iq * bq + at, STRIP), [u for u in strips if u >= at], at)


def _visible():
    return lax.broadcasted_iota(jnp.int32, (STRIP, STRIP), 1) >= lax.broadcasted_iota(jnp.int32, (STRIP, STRIP), 0)


def _forward(q_ref, k_ref, v_ref, o_ref, lse_ref, top_s, mix_s):
    heads, bq, d = q_ref.shape
    scale = d**-0.5
    e = scale * LOG2E
    top_s[...] = jnp.full(top_s.shape, NEG, F32)
    mix_s[...] = jnp.zeros(mix_s.shape, F32)
    ones = jnp.ones((mix_s.shape[1] - d, STRIP), BF)

    def block(key, strips, masked):
        here = pl.ds(key, STRIP)
        pieces = [(i, at) for i in range(heads) for at in strips]
        scores = [_dot(k_ref[i, here, :], q_ref[i, at : at + STRIP, :], 1, 1) for i, at in pieces]
        weights, keeps = [], []
        for (i, at), s in zip(pieces, scores):
            if at == masked:
                s = jnp.where(_visible(), s, HIDDEN)
            old = top_s[i : i + 1, at : at + STRIP]
            top = jnp.maximum(old, s.max(axis=0, keepdims=True))
            top_s[i : i + 1, at : at + STRIP] = top
            weights.append(jnp.exp2((s - top) * e).astype(BF))
            keeps.append(jnp.exp2((old - top) * e))
        for (i, at), p, keep in zip(pieces, weights, keeps):
            values = jnp.concatenate([v_ref[i, here, :].T, ones], axis=0)
            mix_s[i, :, at : at + STRIP] = mix_s[i, :, at : at + STRIP] * keep + _dot(values, p)

    _blocks(block, pl.program_id(0), bq)
    for i in range(heads):
        total = mix_s[i, d : d + 1, :]
        o_ref[i] = (mix_s[i, :d, :] * (1 / total)).T.astype(o_ref.dtype)
        lse_ref[i : i + 1, :] = top_s[i : i + 1, :] * scale + jnp.log(total)


def _params(limit=VMEM, **more):
    return pltpu.CompilerParams(dimension_semantics=("arbitrary",), vmem_limit_bytes=limit, **more)


def _whole(shape):
    return pl.BlockSpec(shape, lambda *_: (0,) * len(shape), pipeline_mode=pl.Buffered(1))


def _cost(flops, *arrays):
    return pl.CostEstimate(flops=flops, transcendentals=0, bytes_accessed=sum(a.size * a.dtype.itemsize for a in arrays))


def attend(q, k, v):
    heads, s, d = q.shape
    bq = min(4 * STRIP, s)
    queries = pl.BlockSpec((heads, bq, d), lambda i: (0, i, 0))
    stats = pl.BlockSpec((heads, bq), lambda i: (0, i))
    return pl.pallas_call(
        _forward,
        grid=(s // bq,),
        in_specs=[queries, _whole(k.shape), _whole(v.shape)],
        out_specs=[queries, stats],
        out_shape=[jax.ShapeDtypeStruct(q.shape, q.dtype), jax.ShapeDtypeStruct((heads, s), F32)],
        scratch_shapes=[pltpu.VMEM((heads, bq), F32), pltpu.VMEM((heads, d + 8, bq), F32)],
        compiler_params=_params(),
        cost_estimate=_cost(4 * q.size * s, q, k, v),
        name="attend",
    )(q, k, v)


def _backward(q_ref, k_ref, v_ref, do_ref, lse_ref, delta_ref, dq_ref, dk_ref, dv_ref, dq_s, dk_s, dv_s):
    heads, bq, d = q_ref.shape
    iq = pl.program_id(0)
    scale = d**-0.5
    e = scale * LOG2E

    @pl.when(iq == 0)
    def _():
        dk_s[...] = jnp.zeros_like(dk_s)
        dv_s[...] = jnp.zeros_like(dv_s)

    dq_s[...] = jnp.zeros_like(dq_s)
    lses = [lse_ref[i : i + 1, :] * LOG2E for i in range(heads)]
    deltas = [delta_ref[i : i + 1, :] for i in range(heads)]

    def block(key, strips, masked):
        here = pl.ds(key, STRIP)
        pieces = [(i, at) for i in range(heads) for at in strips]
        qs = [q_ref[i, at : at + STRIP, :] for i, at in pieces]
        dos = [do_ref[i, at : at + STRIP, :] for i, at in pieces]
        scores = [_dot(k_ref[i, here, :], x, 1, 1) for (i, _), x in zip(pieces, qs)]
        dps = [_dot(v_ref[i, here, :], x, 1, 1) for (i, _), x in zip(pieces, dos)]
        for (i, at), s, dp, x, do in zip(pieces, scores, dps, qs, dos):
            p = jnp.exp2(s * e - lses[i][:, at : at + STRIP])
            if at == masked:
                p = jnp.where(_visible(), p, 0.0)
            ds = (p * (dp - deltas[i][:, at : at + STRIP])).astype(BF)
            dv_s[i, here, :] += _dot(p.astype(BF), do)
            dk_s[i, here, :] += _dot(ds, x)
            dq_s[i, :, at : at + STRIP] += _dot(k_ref[i, here, :].T, ds)

    _blocks(block, iq, bq)
    for i in range(heads):
        dq_ref[i] = (dq_s[i] * scale).T.astype(dq_ref.dtype)

    @pl.when(iq == pl.num_programs(0) - 1)
    def _():
        dk_ref[...] = (dk_s[...] * scale).astype(dk_ref.dtype)
        dv_ref[...] = dv_s[...].astype(dv_ref.dtype)


def attend_bwd(q, k, v, d_out, lse, delta):
    heads, s, d = q.shape
    bq = min(2 * STRIP, s)
    queries = pl.BlockSpec((heads, bq, d), lambda i: (0, i, 0))
    stats = pl.BlockSpec((heads, bq), lambda i: (0, i))
    sums = pltpu.VMEM(k.shape, F32)
    return pl.pallas_call(
        _backward,
        grid=(s // bq,),
        in_specs=[queries, _whole(k.shape), _whole(v.shape), queries, stats, stats],
        out_specs=[queries, _whole(k.shape), _whole(v.shape)],
        out_shape=[jax.ShapeDtypeStruct(q.shape, q.dtype)] * 3,
        scratch_shapes=[pltpu.VMEM((heads, d, bq), F32), sums, sums],
        compiler_params=_params(),
        cost_estimate=_cost(10 * q.size * s, q, k, v, d_out),
        name="attend_bwd",
    )(q, k, v, d_out, lse, delta)


HEAD = 128
THETA = 10000
ROWS = 512


def normed(h):
    wide = h.astype(F32)
    scale = lax.rsqrt(jnp.mean(wide**2, -1, keepdims=True) + 1e-6)
    return (wide * scale).astype(BF)


def normed_bwd(h, ct):
    wide, ct = h.astype(F32), ct.astype(F32)
    scale = lax.rsqrt(jnp.mean(wide**2, -1, keepdims=True) + 1e-6)
    return scale * ct - wide * (scale**3 * jnp.mean(ct * wide, -1, keepdims=True))


def tables(tokens):
    lane = jnp.arange(HEAD, dtype=jnp.int32)
    half = HEAD // 2
    rate = THETA ** (-(lane % half).astype(F32) / half)
    run = 64
    far = (jnp.arange(tokens // run, dtype=F32) * run)[:, None, None] * rate
    near = jnp.arange(run, dtype=F32)[:, None] * rate
    far, near = ((jnp.cos(u), jnp.sin(u)) for u in (far, near))
    (cf, sf), (cn, sn) = lax.optimization_barrier((far, near))
    sin = (sf * cn + cf * sn) * jnp.where(lane < half, -1.0, 1.0)
    return (cf * cn - sf * sn).reshape(tokens, HEAD), sin.reshape(tokens, HEAD)


MESH = pl.DeviceIdType.MESH
HALVES = 2


class Ring:
    def __init__(self):
        me = lax.axis_index("tp")
        self.chips = lax.axis_size("tp") // 2
        self.chip, self.core = me // 2, me % 2
        self.me = me

    def dev(self, k, other=0):
        return (self.chip + k) % self.chips * 2 + (self.core + other) % 2

    def greet(self, others=False):
        barrier = pltpu.get_barrier_semaphore()
        to = [self.dev(0, 1), self.dev(1), self.dev(3)] + ([self.dev(1, 1), self.dev(3, 1)] if others else [])
        for one in to:
            pl.semaphore_signal(barrier, inc=1, device_id={"tp": one}, device_id_type=MESH)
        pl.semaphore_wait(barrier, len(to))


def _table(*rows):
    return tuple(tuple(map(int, row)) for row in rows)


def _remote(src, dst, sems, m, to):
    return pltpu.make_async_remote_copy(src_ref=src, dst_ref=dst, send_sem=sems[0].at[m], recv_sem=sems[1].at[m], device_id={"tp": to},
                                        device_id_type=MESH)


class Gather:
    COPIES = _table("0010", "0130", "0001", "0101", "0110", "0030",
                    "3010", "1130", "3001", "1101",
                    "3101", "1001", "2001", "2101")
    NEXT, CORE, LATER, ON, PASS, FAR, END = range(2), range(2, 4), range(4, 6), range(6, 8), range(8, 10), range(10, 12), range(12, 14)
    EVENTS = ((CORE, ()), (NEXT, (*ON, *PASS)), (PASS, ()), (LATER, FAR), (FAR, ()), (ON, END), (END, ()))

    def __init__(self, ring, own, place, send, recv):
        self.ring, self.own, self.place, self.sem = ring, own, place, (send, recv)

    def copy(self, m):
        k, half, to, other = self.COPIES[m]
        place = self.place(self.ring.dev(k), half)
        return _remote(self.own(half) if k == 0 else place, place, self.sem, m, self.ring.dev(to, other))

    def start(self, *which):
        for m in which:
            self.copy(m).start()

    def arrived(self, *which):
        for m in which:
            k, half, to, other = self.COPIES[m]
            place = self.place(self.ring.dev(k - to, other), half)
            _remote(place, place, self.sem, m, self.ring.dev(to, other)).wait_recv()

    def event(self, i):
        for step, (waits, starts) in enumerate(self.EVENTS):
            @pl.when(i == step)
            def _():
                self.arrived(*waits)
                self.start(*starts)

    def finish(self):
        for m in range(len(self.COPIES)):
            self.copy(m).wait_send()


def places(ring, i):
    p, other = i // 2, i % 2
    off = (p + 1) // 2
    half = p // 2 - p // 3
    return (ring.dev(ring.chips - off, other), half), (ring.dev(off, other), 1 - half)


def _qkv_kernel(own_ref, wq_ref, wk_ref, wv_ref, cos_ref, sin_ref, wg_ref, wu_ref, wd_ref, full_ref, q_ref, k_ref, v_ref, wt_ref, wgt_ref, wut_ref, wdt_ref,
                a_s, cos_s, sin_s, q_s, k_s, v_s, send, recv, in_sem, out_sem, own_sem):
    ring = Ring()
    gather = Gather(ring, lambda half: own_ref.at[half], lambda dev, half: full_ref.at[dev, half], send, recv)
    i = pl.program_id(0)
    slot = i % 2
    heads, r = q_s.shape[1], own_ref.shape[1]
    mine = [pltpu.make_async_copy(a_s.at[0, s], full_ref.at[ring.me, s], own_sem.at[s]) for s in range(HALVES)]

    def loads(i, slot, from_own):
        out = []
        for s, (dev, half) in enumerate(places(ring, i)):
            src = own_ref.at[s] if from_own else full_ref.at[dev, half]
            out += [pltpu.make_async_copy(src, a_s.at[slot, s], in_sem.at[slot, s]),
                    pltpu.make_async_copy(cos_ref.at[dev, half], cos_s.at[slot, s], in_sem.at[slot, 2 + s]),
                    pltpu.make_async_copy(sin_ref.at[dev, half], sin_s.at[slot, s], in_sem.at[slot, 4 + s])]
        return out

    def stores(i, slot):
        return [pltpu.make_async_copy(buf.at[slot, :, s], ref.at[:, dev, half], out_sem.at[slot, 2 * m + s])
                for s, (dev, half) in enumerate(places(ring, i)) for m, (buf, ref) in enumerate(((q_s, q_ref), (k_s, k_ref), (v_s, v_ref)))]

    @pl.when(i == 0)
    def _():
        ring.greet()
        gather.start(*gather.NEXT, *gather.CORE, *gather.LATER)
        for u in loads(i, 0, True):
            u.start()
        for m, w_ref in enumerate((wq_ref, wk_ref, wv_ref)):
            wt_ref[m] = w_ref[...].T

    for w_ref, t_ref in ((wg_ref, wgt_ref), (wu_ref, wut_ref), (wd_ref, wdt_ref)):
        t_ref[...] = w_ref[...].T
    for u in loads(i, slot, False):
        u.wait()

    @pl.when(i == 0)
    def _():
        for u in mine:
            u.start()

    @pl.when(i > 1)
    def _():
        for u in stores(i - 2, slot):
            u.wait()

    a = a_s[slot].reshape(HALVES * r, -1)
    cos, sin = cos_s[slot].reshape(-1, HEAD), sin_s[slot].reshape(-1, HEAD)
    for w_ref, out_s in ((wq_ref, q_s), (wk_ref, k_s), (wv_ref, v_s)):
        t = _dot(a, w_ref[...], 1, 0).astype(BF)
        for n in range(heads):
            one = t[:, n * HEAD : (n + 1) * HEAD]
            if out_s is not v_s:
                wide = one.astype(F32)
                one = (wide * cos + pltpu.roll(wide, HEAD // 2, 1) * sin).astype(BF)
            out_s[slot, n] = one.reshape(HALVES, r, HEAD)
    for u in stores(i, slot):
        u.start()

    @pl.when(i == 0)
    def _():
        for u in mine:
            u.wait()

    gather.event(i)

    @pl.when(i < STEPS - 1)
    def _():
        for u in loads(i + 1, 1 - slot, False):
            u.start()

    @pl.when(i == STEPS - 1)
    def _():
        for u in stores(i - 1, 1 - slot) + stores(i, slot):
            u.wait()
        gather.finish()


STEPS = 8
ANY = pl.BlockSpec(memory_space=pl.ANY)


def qkv(own, ws, cos, sin, turn):
    devices, _, r, _ = cos.shape
    d = own.shape[1]
    heads = ws[0].shape[1] // HEAD
    shape = jax.ShapeDtypeStruct((heads, devices, HALVES, r, HEAD), BF)
    full = jax.ShapeDtypeStruct((devices, HALVES, r, d), BF)
    wt = (len(ws), *ws[0].shape[::-1])
    dma = pltpu.SemaphoreType.DMA
    copies = len(Gather.COPIES)
    return pl.pallas_call(
        _qkv_kernel,
        grid=(STEPS,),
        in_specs=[ANY, *(_whole(w.shape) for w in ws), ANY, ANY, *(pl.BlockSpec((w.shape[0], w.shape[1] // STEPS), lambda i: (0, i)) for w in turn)],
        out_specs=[ANY] * 4 + [_whole(wt), *(pl.BlockSpec((w.shape[1] // STEPS, w.shape[0]), lambda i: (i, 0)) for w in turn)],
        out_shape=[full, shape, shape, shape, *(jax.ShapeDtypeStruct(u, BF) for u in (wt, *(w.shape[::-1] for w in turn)))],
        scratch_shapes=[pltpu.VMEM((2, HALVES, r, d), BF), *[pltpu.VMEM((2, HALVES, r, HEAD), F32)] * 2,
                        *[pltpu.VMEM((2, heads, HALVES, r, HEAD), BF)] * 3, dma((copies,)), dma((copies,)), dma((2, 6)), dma((2, 6)), dma((2,))],
        compiler_params=_params(collective_id=0, has_side_effects=True),
        cost_estimate=_cost(6 * devices * own.size * ws[0].shape[1], own, *ws),
        name="gather_qkv",
    )(own.reshape(HALVES, r, d), *ws, cos, sin, *turn)


SPOTS = (_table("000", "001"), _table("010", "011"), _table("300", "100"), _table("310", "110"), _table("200", "210"),
         _table("301", "101"), _table("311", "111"), _table("201", "211"))


def _ffn_kernel(own_ref, dy_own, dy_first, wg_in, wu_in, wdt_in, wgt_in, wut_in, full_ref, dy_ref, hid_ref, dg_ref, du_ref, db_ref,
                b_s, dy_s, hid_s, dg_s, du_s, db_s, wg_ref, wu_ref, wdt_ref, wgt_ref, wut_ref, *sems):
    *sems, in_sem, out_sem, own_sem, w_sem = sems
    ring = Ring()
    first, second, dys = (Gather(ring, lambda q, own=own, half=half: own.at[half, q], lambda dev, q, full=full, half=half: full.at[dev, half, q], *pair)
                          for own, full, half, pair in ((own_ref, full_ref, 0, sems[:2]), (own_ref, full_ref, 1, sems[2:4]), (dy_own, dy_ref, 1, sems[4:])))
    i = pl.program_id(0)
    slot = i % 2
    rows = hid_s.shape[1] * hid_s.shape[2]
    weights = [pltpu.make_async_copy(src, dst, w_sem.at[m]) for m, (src, dst) in enumerate(
        ((wg_in, wg_ref), (wu_in, wu_ref), (wdt_in, wdt_ref), (wgt_in, wgt_ref), (wut_in, wut_ref)))]

    def loads(step):
        out = []
        for s, (k, other, half) in enumerate(SPOTS[step]):
            dev = ring.dev(k, other)
            mine = k == other == 0
            dy = (dy_own.at[half] if mine else dy_ref.at[dev, half]) if half else dy_first.at[dev]
            out += [pltpu.make_async_copy(own_ref.at[half] if mine else full_ref.at[dev, half], b_s.at[step % 2, s], in_sem.at[step % 2, s]),
                    pltpu.make_async_copy(dy, dy_s.at[step % 2, s], in_sem.at[step % 2, 2 + s])]
        return out

    def kept(step):
        out = []
        for s, (k, other, half) in enumerate(SPOTS[step]):
            dev = ring.dev(k, other)
            if k == other == 0:
                out.append(pltpu.make_async_copy(b_s.at[step % 2, s], full_ref.at[dev, half], own_sem.at[s]))
            if k == other == 0 or half == 0:
                out.append(pltpu.make_async_copy(dy_s.at[step % 2, s], dy_ref.at[dev, half], own_sem.at[2 + s]))
        return out

    def stores(step):
        return [pltpu.make_async_copy(buf.at[step % 2, s], ref.at[ring.dev(k, other), half], out_sem.at[step % 2, 2 * m + s])
                for s, (k, other, half) in enumerate(SPOTS[step])
                for m, (buf, ref) in enumerate(((hid_s, hid_ref), (dg_s, dg_ref), (du_s, du_ref), (db_s, db_ref)))]

    def arrivals(step):
        if step == 0:
            for one in (first, second, dys):
                one.arrived(*one.CORE)
        if step == 1:
            first.arrived(*first.NEXT)
            first.start(*first.ON, *first.PASS)
            first.arrived(*first.LATER)
            first.start(*first.FAR)
            for one in (second, dys):
                one.start(*one.NEXT, *one.LATER)
        if step == 2:
            first.arrived(*first.ON)
            first.start(*first.END)
            first.arrived(*first.PASS, *first.FAR)
        if step == 3:
            first.arrived(*first.END)
        if step == 4:
            for one in (second, dys):
                one.arrived(*one.NEXT)
                one.start(*one.ON, *one.PASS)
                one.arrived(*one.LATER)
                one.start(*one.FAR)
        if step == 5:
            for one in (second, dys):
                one.arrived(*one.PASS, *one.FAR)
        if step == 6:
            for one in (second, dys):
                one.arrived(*one.ON)
                one.start(*one.END)
            for one in (second, dys):
                one.arrived(*one.END)

    @pl.when(i == 0)
    def _():
        ring.greet()
        first.start(*first.NEXT, *first.CORE, *first.LATER)
        second.start(*second.CORE)
        dys.start(*dys.CORE)
        for u in loads(0) + weights:
            u.start()
        for u in weights[:3]:
            u.wait()

    for step in range(STEPS):
        @pl.when(i == step)
        def _():
            for u in loads(step):
                u.wait()
            for u in kept(step):
                u.start()

    b = b_s[slot].reshape(rows, -1)
    gate = _dot(b, wg_ref[...])
    up = _dot(b, wu_ref[...])
    dh = _dot(dy_s[slot].reshape(rows, -1), wdt_ref[...]).astype(BF).astype(F32)

    for step in range(STEPS):
        @pl.when(i == step)
        def _():
            for u in kept(step) + (weights[3:] if step == 0 else []) + (stores(step - 2) if step > 1 else []):
                u.wait()
            arrivals(step)
            for u in loads(step + 1) if step + 1 < STEPS else ():
                u.start()

    s = 1 / (1 + jnp.exp(-gate))
    silu = gate * s
    hid_s[slot] = (silu * up).astype(BF).reshape(hid_s.shape[1:])
    dg = (dh * up * (s * (1 + gate * (1 - s)))).astype(BF)
    du = (dh * silu).astype(BF)
    dg_s[slot] = dg.reshape(dg_s.shape[1:])
    du_s[slot] = du.reshape(du_s.shape[1:])
    db_s[slot] = (_dot(dg, wgt_ref[...]) + _dot(du, wut_ref[...])).astype(BF).reshape(db_s.shape[1:])

    for step in range(STEPS):
        @pl.when(i == step)
        def _():
            for u in stores(step):
                u.start()

    @pl.when(i == STEPS - 1)
    def _():
        for step in (STEPS - 2, STEPS - 1):
            for u in stores(step):
                u.wait()
        for one in (first, second, dys):
            one.finish()


def ffn(own, dy, dy_first, wg, wu, wgt, wut, wdt):
    t, d = own.shape
    r = t // HALVES
    devices = dy_first.shape[0] // r
    f = wg.shape[1]
    q = (HALVES, r // HALVES, d)
    array = lambda k: jax.ShapeDtypeStruct((devices, HALVES, r, k), BF)
    full = jax.ShapeDtypeStruct((devices, HALVES, *q), BF)
    dma = pltpu.SemaphoreType.DMA
    return pl.pallas_call(
        _ffn_kernel,
        grid=(STEPS,),
        in_specs=[ANY] * 8,
        out_specs=[ANY] * 6,
        out_shape=[full, full, array(f), array(f), array(f), array(d)],
        scratch_shapes=[*[pltpu.VMEM((2, HALVES, *q), BF)] * 2, *[pltpu.VMEM((2, HALVES, r, f), BF)] * 3, pltpu.VMEM((2, HALVES, r, d), BF),
                        *(pltpu.VMEM(w.shape, BF) for w in (wg, wu, wdt, wgt, wut)),
                        *[dma((len(Gather.COPIES),))] * 6, dma((2, 4)), dma((2, 8)), dma((4,)), dma((5,))],
        compiler_params=_params(collective_id=1, has_side_effects=True),
        cost_estimate=_cost(10 * devices * dy.size * f, own, dy_first, wg, wu, wdt),
        name="gather_ffn",
    )(own.reshape(HALVES, *q), dy.reshape(HALVES, *q), dy_first.reshape(devices, *q), wg, wu, wdt, wgt, wut)


class Scatter:
    SENDS = (*_table("201"), *_table("213"), *_table("1110", "3031", "1010", "3131"))
    ORDER = _table("20", "21", "11", "30", "10", "31", "00", "01")
    COPIES = 8 + len(SENDS)

    def __init__(self, ring, part, pair, relay, last, own, send, recv, load):
        self.ring, self.part, self.pair, self.own, self.sem, self.load = ring, part, pair, own, (send, recv), load
        self.buffers = {"relay": relay, "last": last}

    def copy(self, m):
        if m < len(self.ORDER):
            k, half = self.ORDER[m]
            return _remote(self.part.at[self.ring.dev(k, 1), half], self.pair.at[k, half], self.sem, m, self.ring.dev(0, 1))
        k, half, to, *side = self.SENDS[m - len(self.ORDER)]
        dst = self.buffers["last"].at[side[0], half] if side else self.buffers["relay"].at[half]
        return _remote(self.pair.at[k, half], dst, self.sem, m, self.ring.dev(to))

    def own_load(self, m):
        k, half = self.ORDER[m]
        return pltpu.make_async_copy(self.part.at[self.ring.dev(k), half], self.own.at[m % 2], self.load.at[m % 2])

    def begin(self):
        self.ring.greet()
        for m in range(8):
            self.copy(m).start()
        for m in range(2):
            self.own_load(m).start()

    def add(self, m, relayed=None):
        k, half = self.ORDER[m]
        self.copy(m).wait_recv()
        self.own_load(m).wait()
        if relayed is not None:
            self.copy(8 + relayed).wait_recv()
        rows = 32

        def some(j, _):
            here = pl.ds(pl.multiple_of(j * rows, rows), rows)
            total = self.pair[k, half, here].astype(F32) + self.own[m % 2, here].astype(F32)
            if relayed is not None:
                total += self.buffers["relay"][relayed, here].astype(F32)
            self.pair[k, half, here] = total.astype(BF)

        lax.fori_loop(0, self.pair.shape[2] // rows, some, None)
        if m + 2 < 8:
            self.own_load(m + 2).start()

    def first(self):
        for m in range(4):
            self.add(m)
            self.copy(8 + m).start()

    def second(self):
        for m in (4, 5):
            self.add(m, m - 4)
            self.copy(8 + m).start()

    def final(self, out):
        last = self.buffers["last"]
        for half in range(HALVES):
            m = 6 + half
            self.copy(m).wait_recv()
            self.own_load(m).wait()
            self.copy(12 - 2 * half).wait_recv()
            self.copy(11 + 2 * half).wait_recv()
            rows = 32

            def some(j, _):
                here = pl.ds(pl.multiple_of(j * rows, rows), rows)
                total = self.pair[0, half, here].astype(F32) + self.own[m % 2, here].astype(F32)
                out[half, here] = (total + last[0, half, here].astype(F32) + last[1, half, here].astype(F32)).astype(BF)

            lax.fori_loop(0, self.pair.shape[2] // rows, some, None)
        for m in range(self.COPIES):
            self.copy(m).wait_send()


def _scatter_kernel(part_ref, *refs, groups, relay_step):
    outs = sum(len(flips) for _, flips in groups)
    ins = len(groups) + outs
    given, results, out_ref, scratch = refs[:ins], refs[ins : ins + outs], refs[ins + outs], refs[ins + outs + 1 :]
    *scratch, whole_sem = scratch
    scratch, wholes = scratch[:-outs], list(scratch[-outs:])
    ring = Ring()
    scatter = Scatter(ring, part_ref, *scratch)
    i = pl.program_id(0)
    copies, at = [], 0
    for _, flips in groups:
        for m in range(len(flips)):
            copies.append(pltpu.make_async_copy(given[at + 1 + m], wholes[len(copies)], whole_sem.at[len(copies)]))
        at += 1 + len(flips)

    @pl.when(i == 0)
    def _():
        scatter.begin()
        for u in copies:
            u.start()
        scatter.first()
        for u in copies:
            u.wait()

    @pl.when(i == relay_step)
    def _():
        scatter.second()

    first = at = to = 0
    for steps, flips in groups:
        s_ref, r_refs = given[at], wholes[to : to + len(flips)]
        at, results_here, to = at + 1 + len(flips), results[to : to + len(flips)], to + len(flips)

        @pl.when((i >= first) & (i < first + steps))
        def _():
            for r_ref, o_ref, flip in zip(r_refs, results_here, flips):
                left, right = (r_ref, s_ref) if flip else (s_ref, r_ref)

                def some(cols, left=left, right=right, o_ref=o_ref):
                    o_ref[cols, :] = _dot(left[:, cols].T, right[...]).astype(BF)

                _by_rows(left.shape[1], some, STRIP // 2)

        first += steps

    @pl.when(i == pl.num_programs(0) - 1)
    def _():
        scatter.final(out_ref)


def scattered_beside(part, products, tile, relay_step, collective_id, name):
    devices, _, r, d = part.shape
    groups, given, specs, wholes, out_specs, out_shape, first, flops = [], [], [], [], [], [], 0, 0
    for s, others in products:
        t, n = s.shape
        steps = n // tile
        at = lambda i, first=first, steps=steps: jnp.clip(i - first, 0, steps - 1)
        given.append(s)
        specs.append(pl.BlockSpec((t, tile), lambda i, at=at: (0, at(i))))
        for u, flip in others:
            k = u.shape[1]
            given.append(u)
            specs.append(ANY)
            wholes.append(pltpu.VMEM(u.shape, BF))
            out_shape.append(jax.ShapeDtypeStruct((k, n) if flip else (n, k), BF))
            out_specs.append(pl.BlockSpec((k, tile), lambda i, at=at: (0, at(i))) if flip else pl.BlockSpec((tile, k), lambda i, at=at: (at(i), 0)))
            flops += 2 * t * n * k
        groups.append((steps, tuple(flip for _, flip in others)))
        first += steps
    dma = pltpu.SemaphoreType.DMA
    *results, rows = pl.pallas_call(
        functools.partial(_scatter_kernel, groups=tuple(groups), relay_step=relay_step),
        grid=(first,),
        in_specs=[ANY, *specs],
        out_specs=[*out_specs, pl.BlockSpec((HALVES, r, d), lambda i: (0, 0, 0))],
        out_shape=[*out_shape, jax.ShapeDtypeStruct((HALVES, r, d), BF)],
        scratch_shapes=[pltpu.VMEM((4, HALVES, r, d), BF), pltpu.VMEM((2, r, d), BF), pltpu.VMEM((2, HALVES, r, d), BF), pltpu.VMEM((2, r, d), BF),
                        dma((Scatter.COPIES,)), dma((Scatter.COPIES,)), dma((2,)), *wholes, dma((len(wholes),))],
        compiler_params=_params(63 * MIB, collective_id=collective_id, has_side_effects=True),
        cost_estimate=_cost(flops, part, *given),
        name=name,
    )(part, *given)
    return rows, results


class Exchange:
    NEAR = _table("01", "10", "11", "30", "31")
    FAR = _table("010", "011", "130", "131")
    COPIES = len(NEAR) + 2 * len(FAR)

    def __init__(self, ring, piece, land, relay, send, recv):
        self.ring, self.piece, self.land, self.relay, self.sem = ring, piece, land, relay, (send, recv)
        self.part = relay.shape[2]

    def near(self, m):
        to = self.ring.dev(*self.NEAR[m])
        return _remote(self.piece(to), self.land(self.ring.me), self.sem, m, to)

    def some(self, ref, side):
        return ref.at[pl.ds(side * self.part, self.part)]

    def far(self, m):
        side, k, other = self.FAR[m]
        return _remote(self.some(self.piece(self.ring.dev(2, other)), side), self.relay.at[side, other], self.sem, len(self.NEAR) + m, self.ring.dev(k))

    def on(self, m):
        side, k, other = self.FAR[m]
        return _remote(self.relay.at[side, other], self.some(self.land(self.ring.dev(-k)), side), self.sem,
                       len(self.NEAR) + len(self.FAR) + m, self.ring.dev(k, other))

    def begin(self, k):
        for m in range(len(self.FAR)) if k == 2 else ():
            self.far(m).start()
        for m, (chips, _) in enumerate(self.NEAR):
            if chips == k:
                self.near(m).start()

    def send_on(self):
        for m in range(len(self.FAR)):
            self.far(m).wait_recv()
            self.on(m).start()

    def arrived(self, k):
        for m, (chips, other) in enumerate(self.NEAR):
            if (chips + k) % 4 == 0:
                place = self.land(self.ring.dev(k, other))
                _remote(place, place, self.sem, m, self.ring.dev(chips, other)).wait_recv()
        for m, (side, chips, other) in enumerate(self.FAR if k == 2 else ()):
            place = self.some(self.land(self.ring.dev(2, other)), side)
            _remote(place, place, self.sem, len(self.NEAR) + len(self.FAR) + m, self.ring.dev(chips, other)).wait_recv()

    def finish(self):
        for m in range(len(self.NEAR)):
            self.near(m).wait_send()
        for m in range(len(self.FAR)):
            self.far(m).wait_send()
            self.on(m).wait_send()


ONE = 64
CHIPS = (2, 1, 3, 0)


def _by_rows(total, act, one=ONE):
    lax.fori_loop(0, total // one, lambda j, _: act(pl.ds(pl.multiple_of(j * one, one), one)), None)


def _wo_kernel(o_ref, wo_ref, x_ref, mine_ref, h_ref, b_ref, land_s, relay_s, wo_s, sum_s, send, recv, here):
    ring = Ring()
    heads, t = land_s.shape[1], land_s.shape[2]
    exchange = Exchange(ring, lambda dev: o_ref.at[:, dev], lambda dev: land_s.at[dev], relay_s, send, recv)
    own = pltpu.make_async_copy(o_ref.at[:, ring.me], land_s.at[ring.me], here.at[0])
    whole = pltpu.make_async_copy(wo_ref, wo_s, here.at[1])
    whole.start()
    own.start()
    ring.greet(True)
    for k in CHIPS:
        exchange.begin(k)
    whole.wait()
    own.wait()
    wide = 2 * heads * HEAD
    sum_s[...] = jnp.zeros(sum_s.shape, F32)

    def add(j, _):
        k = j + j // 2 - j // 3 * 2
        for one in range(4):
            @pl.when(k == one)
            def _():
                exchange.arrived(one)
                if one == 0:
                    exchange.send_on()
        chip = (ring.chip + k) % ring.chips
        cols = pl.ds(pl.multiple_of(chip * wide, wide), wide)
        mine_ref[:, cols] = jnp.concatenate([land_s[chip * 2 + core, n] for core in range(2) for n in range(heads)], axis=1)
        sum_s[...] += _dot(mine_ref[:, cols], wo_s[cols, :])

    lax.fori_loop(0, ring.chips, add, None)

    def last(rows):
        h = (x_ref[rows].astype(F32) + sum_s[rows].astype(BF).astype(F32)).astype(BF)
        h_ref[rows] = h
        b_ref[rows] = normed(h)

    _by_rows(t, last)
    exchange.finish()


def exchange_wo(o, wo, x):
    heads, devices, t, _ = o.shape
    d = x.shape[1]
    dma = pltpu.SemaphoreType.DMA
    return pl.pallas_call(
        _wo_kernel,
        in_specs=[ANY, ANY, pl.BlockSpec(memory_space=pltpu.VMEM)],
        out_specs=[pl.BlockSpec(memory_space=pltpu.VMEM)] * 3,
        out_shape=[jax.ShapeDtypeStruct((t, wo.shape[0]), BF), *[jax.ShapeDtypeStruct(x.shape, BF)] * 2],
        scratch_shapes=[pltpu.VMEM((devices, heads, t, HEAD), BF), pltpu.VMEM((2, 2, heads // 2, t, HEAD), BF), pltpu.VMEM(wo.shape, BF),
                        pltpu.VMEM((t, d), F32), dma((Exchange.COPIES,)), dma((Exchange.COPIES,)), dma((2,))],
        compiler_params=pltpu.CompilerParams(vmem_limit_bytes=VMEM, collective_id=4, has_side_effects=True),
        cost_estimate=_cost(2 * t * wo.size, o, x, wo),
        name="exchange_wo",
    )(o, wo, x)


def _dwo_kernel(wo_ref, db_ref, h_ref, dy_ref, mine_ref, dh_ref, do_ref, dwo_ref, out_s, relay_s, wo_s, dwo_s, send, recv, here):
    ring = Ring()
    heads, t = out_s.shape[1], out_s.shape[2]
    exchange = Exchange(ring, lambda dev: out_s.at[dev], lambda dev: do_ref.at[:, dev], relay_s, send, recv)
    own = pltpu.make_async_copy(out_s.at[ring.me], do_ref.at[:, ring.me], here.at[0])
    whole = pltpu.make_async_copy(wo_ref, wo_s, here.at[1])
    whole.start()
    ring.greet(True)

    def first(rows):
        dh_ref[rows] = (dy_ref[rows].astype(F32) + normed_bwd(h_ref[rows], db_ref[rows]).astype(BF).astype(F32)).astype(BF)

    _by_rows(t, first)
    whole.wait()
    wide = 2 * heads * HEAD

    def give(j, _):
        k = (2 - j + ring.chips) % ring.chips
        chip = (ring.chip + k) % ring.chips
        part = _dot(dh_ref[...], wo_s[pl.ds(pl.multiple_of(chip * wide, wide), wide), :], 1, 1).astype(BF)
        for m in range(2 * heads):
            out_s[chip * 2 + m // heads, m % heads] = part[:, m * HEAD : (m + 1) * HEAD]
        for one in CHIPS:
            @pl.when(k == one)
            def _():
                exchange.begin(one)

    lax.fori_loop(0, ring.chips, give, None)
    own.start()
    store = lambda m, tile: pltpu.make_async_copy(dwo_s.at[tile], dwo_ref.at[tile], here.at[2 + m])
    tiles = dwo_s.shape[0] // wide

    def term(m, _):
        tile = pl.ds(pl.multiple_of(m * wide, wide), wide)
        dwo_s[tile] = _dot(mine_ref[:, tile].T, dh_ref[...]).astype(BF)
        store(m, tile).start()

    lax.fori_loop(0, 1, term, None)
    exchange.send_on()
    lax.fori_loop(1, tiles, term, None)
    stores = [store(m, pl.ds(m * wide, wide)) for m in range(tiles)]
    for k in CHIPS:
        exchange.arrived(k)
    for u in (own, *stores):
        u.wait()
    exchange.finish()


def exchange_dwo(wo, db, h, dy, mine, heads):
    t, d = h.shape
    devices = wo.shape[0] // heads // HEAD
    dma = pltpu.SemaphoreType.DMA
    vmem = pl.BlockSpec(memory_space=pltpu.VMEM)
    return pl.pallas_call(
        _dwo_kernel,
        in_specs=[ANY, *[vmem] * 4],
        out_specs=[vmem, ANY, ANY],
        out_shape=[jax.ShapeDtypeStruct(h.shape, BF), jax.ShapeDtypeStruct((heads, devices, t, HEAD), BF), jax.ShapeDtypeStruct(wo.shape, BF)],
        scratch_shapes=[pltpu.VMEM((devices, heads, t, HEAD), BF), pltpu.VMEM((2, 2, heads // 2, t, HEAD), BF), pltpu.VMEM(wo.shape, BF),
                        pltpu.VMEM(wo.shape, BF), dma((Exchange.COPIES,)), dma((Exchange.COPIES,)), dma((2 + devices // 2,))],
        compiler_params=pltpu.CompilerParams(vmem_limit_bytes=VMEM, collective_id=5, has_side_effects=True),
        cost_estimate=_cost(4 * t * wo.size, wo, wo),
        name="exchange_dwo",
    )(wo, db, h, dy, mine)


def _da_kernel(dq_ref, dk_ref, dv_ref, cos_ref, sin_ref, wt_ref, g_ref, da_ref):
    rows = g_ref.shape[0]
    cos, sin = cos_ref[...].reshape(rows, HEAD), sin_ref[...].reshape(rows, HEAD)
    heads = dq_ref.shape[0]
    for m, ref in enumerate((dq_ref, dk_ref, dv_ref)):
        for n in range(heads):
            one = ref[n].reshape(rows, HEAD)
            if ref is not dv_ref:
                wide = one.astype(F32)
                one = (wide * cos - pltpu.roll(wide, HEAD // 2, 1) * sin).astype(BF)
            g_ref[:, (m * heads + n) * HEAD : (m * heads + n + 1) * HEAD] = one
    da_ref[...] = _dot(g_ref[...], wt_ref[...], 1, 0).astype(BF)


def da_of(dq, dk, dv, cos, sin, wt):
    heads, t, _ = dq.shape
    k, d = wt.shape
    place = pl.BlockSpec((ROWS, HEAD), lambda i: (i, 0))
    return pl.pallas_call(
        _da_kernel,
        grid=(t // ROWS,),
        in_specs=[pl.BlockSpec((heads, ROWS, HEAD), lambda i: (0, i, 0))] * 3 + [place, place, _whole(wt.shape)],
        out_specs=[pl.BlockSpec((ROWS, k), lambda i: (i, 0)), pl.BlockSpec((ROWS, d), lambda i: (i, 0))],
        out_shape=[jax.ShapeDtypeStruct((t, k), BF), jax.ShapeDtypeStruct((t, d), BF)],
        compiler_params=_params(),
        cost_estimate=_cost(2 * t * k * d, wt),
        name="da",
    )(dq, dk, dv, cos, sin, wt)


def gathered(t):
    return lax.all_gather(t, "tp", axis=0, tiled=True)


def scattered(t):
    return lax.psum_scatter(t, "tp", scatter_dimension=0, tiled=True)


def after(t, *first):
    return lax.optimization_barrier((t, *first))[0]


def layer(x, dy, wq, wk, wv, wo, wg, wu, wd):
    t, d = x.shape
    n = lax.axis_size("tp")
    r = t // HALVES
    tokens = n * t
    table = tables(tokens)
    flat = lambda u: u.reshape(tokens, -1)

    a, *q, wt, wgt, wut, wdt = qkv(normed(x), (wq, wk, wv), *(u.reshape(n, HALVES, r, HEAD) for u in table), (wg, wu, wd))
    q, k, v = (u.reshape(-1, tokens, HEAD) for u in q)
    heads = len(q)
    whole_wo = gathered(wo)
    dy_first = gathered(after(dy[:r], a))
    out, lse = attend(q, k, v)
    mine, h, b = exchange_wo(out.reshape(heads, n, t, HEAD), whole_wo, x)

    b, dys, hid, dg, du, db = ffn(b, dy, dy_first, wg, wu, wgt, wut, wdt)
    db, (dwg, dwu) = scattered_beside(db, ((flat(b), ((flat(dg), False), (flat(du), False))),), 512, 3, 2, "scatter_db")
    dh, dout, dwo = exchange_dwo(whole_wo, db.reshape(t, d), h, dy, mine, heads)
    dwo = scattered(dwo)
    dout = dout.reshape(heads, tokens, HEAD)
    delta = (dout.astype(F32) * out.astype(F32)).sum(-1)
    g, da = da_of(*attend_bwd(q, k, v, dout, lse, delta), *table, wt.reshape(-1, d))
    da, (dwd, dwqkv) = scattered_beside(da.reshape(n, HALVES, r, d), ((flat(dys), ((flat(hid), True),)), (flat(a), ((g, False),))), 512, 5, 3, "scatter_da")
    dx = dh + normed_bwd(x, da.reshape(t, d)).astype(BF)
    dwq, dwk, dwv = jnp.split(dwqkv, 3, axis=1)
    return dx, dwq, dwk, dwv, dwo, dwg, dwu, dwd


def solution(mesh):
    def step(x, dy, *weights):
        dx, *dw = layer(x[0], dy[0], *weights)
        return (dx[None], *dw)

    states, by_columns, by_rows = P("dp", "tp", None), P(None, "tp"), P("tp", None)
    weights = (by_columns, by_columns, by_columns, by_rows, by_columns, by_columns, by_rows)
    own = tuple(P("dp", "tp") if spec == by_columns else P(("dp", "tp"), None) for spec in weights)
    return jax.shard_map(step, mesh=mesh, in_specs=(states, states, *weights), out_specs=(states, *own), check_vma=False)
```
